32 devices in a mesh: tm: 16 (over z, x, core), chan: 2 (over y).
Axes of the slice: x: 2, y: 2, z: 4, core: 2. Of those that a mesh axis runs over, the one named last changes fastest.
Arguments:
- trans: float32 [4, 128, 32768], P(None, 'chan', 'tm'), may hold values from -1 to 1
- drive: float32 [2, 128, 32768], P(None, 'chan', 'tm'), may hold values from -60 to 60
- back_drive: float32 [2, 128, 32768], P(None, 'chan', 'tm'), may hold values from -60 to 60
- readout: float32 [128, 2, 128], P('chan'), may hold values from -0.375 to 0.375
Outputs:
- observed: float32 [128, 32768], P('chan', 'tm')
The draws below stay inside these ranges and needn't reach their ends.
All inputs are finite; a program needn't handle non-finite values.
Results may differ from the reference program's by a relative error of at most 0.0003.
Values sent between devices are 32-bit elements; how exact they have to be, the bound alone decides.
No kernel may reach another device: no remote copies, remote signals or barrier semaphores. Data moves between devices by JAX's collectives and lax.ppermute only.
A program may use at most 64 MiB of HBM per device.

```python
import math
import jax
import jax.numpy as jnp
from jax import lax

CH = 128
TS_DEV = 2048
TOTAL_TIMESTEPS = 32768


def draw_trans(key, part):
    share = 0.5
    slow = jax.random.uniform(jax.random.fold_in(key, 1), (CH,)) < share
    slow_rate = 0.6 / TOTAL_TIMESTEPS * jnp.exp(jax.random.uniform(jax.random.fold_in(key, 2), (CH,), jnp.float32, -0.3, 0.3))
    fast_rate = 1.0 / jax.random.uniform(jax.random.fold_in(key, 3), (CH,), jnp.float32, 30.0, 50.0)
    base_level = jnp.where(slow, slow_rate, fast_rate)[:, None]
    block_count = TOTAL_TIMESTEPS // TS_DEV
    block_factor = jnp.exp(jax.random.uniform(jax.random.fold_in(key, 4), (CH, block_count), jnp.float32, math.log(0.5), math.log(2.0)))
    block_complete = jnp.repeat(block_factor, TS_DEV, axis=1)
    per_step_multiplier = jax.random.uniform(jax.random.fold_in(key, 5), (CH, TOTAL_TIMESTEPS), jnp.float32, 0.5, 1.5)
    spike_locations = jax.random.randint(jax.random.fold_in(key, 6), (3,), 0, TOTAL_TIMESTEPS)
    step_positions = jnp.arange(TOTAL_TIMESTEPS)
    spike_events = jnp.sum((step_positions[None, :] == spike_locations[:, None]).astype(jnp.float32), axis=0) * 0.5
    decay_factor = base_level * block_complete * per_step_multiplier + spike_events[None, :]
    scale = jnp.exp(-decay_factor)
    angle = jax.random.uniform(jax.random.fold_in(key, 7), (CH, TOTAL_TIMESTEPS), jnp.float32, -math.pi, math.pi)
    cosine = scale * jnp.cos(angle)
    sine = scale * jnp.sin(angle)
    return jnp.stack([cosine, -sine, sine, cosine], axis=0).astype(jnp.float32)


def common_drive(key):
    ramp = 1.0 + 2.0 * jnp.arange(TOTAL_TIMESTEPS).astype(jnp.float32) / (TOTAL_TIMESTEPS - 1)
    values = jax.random.truncated_normal(jax.random.fold_in(key, 3), -5.0, 5.0, (2, CH, TOTAL_TIMESTEPS), jnp.float32)
    return (values * ramp[None, None, :]).astype(jnp.float32)


def draw_drive(key, part):
    return common_drive(jax.random.fold_in(key, 11))


def draw_back_drive(key, part):
    return common_drive(jax.random.fold_in(key, 12))


def shard_levels(stream_key, extent, pieces, least, largest):
    gain = 1.0
    for position, parts in pieces:
        draws = jax.random.uniform(jax.random.fold_in(jax.random.fold_in(stream_key, 6), position), (parts,), jnp.float32, least / len(pieces), largest / len(pieces))
        gain = gain * jnp.repeat(jnp.exp(draws), extent[position] // parts).reshape((-1,) + (1,) * (len(extent) - 1 - position))
    return gain


def bell_draw(key, dims, scale, most, cuts=(), kind=jnp.bfloat16):
    values = scale * jax.random.normal(key, dims, jnp.float32)
    if cuts:
        values = values * shard_levels(key, dims, cuts, -0.22, 0.18)
    return jnp.clip(values, -most, most).astype(kind)


def setup_inputs(seed: int = 0) -> dict:
    arg_keys = jax.random.split(jax.random.key(seed), 5)
    return {
        "trans": draw_trans(jax.random.fold_in(arg_keys[4], 71), 0),
        "drive": draw_drive(jax.random.fold_in(arg_keys[4], 71), 0),
        "back_drive": draw_back_drive(jax.random.fold_in(arg_keys[4], 71), 0),
        "readout": bell_draw(arg_keys[3], (CH, 2, CH), (2 * CH) ** -0.5, 0.375, ((0, 2),), jnp.float32),
    }


epsilon = 1e-06

def forward_step(state, inputs):
    matrix, source = inputs
    first = matrix[0] * state[0] + matrix[1] * state[1] + source[0]
    second = matrix[2] * state[0] + matrix[3] * state[1] + source[1]
    result = jnp.stack([first, second], axis=0)
    return (result, result)

def backward_step(state, inputs):
    matrix, source = inputs
    first = matrix[0] * state[0] + matrix[2] * state[1] + source[0]
    second = matrix[1] * state[0] + matrix[3] * state[1] + source[1]
    result = jnp.stack([first, second], axis=0)
    return (result, result)

def reference(trans, drive, back_drive, readout):
    matrices = jnp.moveaxis(trans, 2, 0)
    sources = jnp.moveaxis(drive, 2, 0)
    back_sources = jnp.moveaxis(back_drive, 2, 0)
    start = jnp.zeros((2, CH), trans.dtype)
    _, forward_states = lax.scan(forward_step, start, (matrices, sources))
    _, backward_states = lax.scan(backward_step, start, (matrices, back_sources), reverse=True)
    count = 2.0 * TOTAL_TIMESTEPS
    norm_f = jnp.sqrt(lax.optimization_barrier(jnp.sum(forward_states * forward_states, axis=(0, 1))) / count + epsilon)
    norm_b = jnp.sqrt(lax.optimization_barrier(jnp.sum(backward_states * backward_states, axis=(0, 1))) / count + epsilon)
    smoothed = forward_states / norm_f + backward_states / norm_b
    smoothed = jnp.moveaxis(smoothed, 0, 2).reshape(2 * CH, TOTAL_TIMESTEPS)
    return jnp.dot(readout.reshape(CH, 2 * CH), smoothed, precision=lax.Precision.HIGHEST, preferred_element_type=jnp.float32)
```

```python
import jax
import jax.numpy as jnp
from jax import lax
from jax.experimental import pallas as pl
from jax.experimental.pallas import tpu as pltpu
from jax.sharding import PartitionSpec as P

epsilon = 1e-06
LANES = 128
SUBS = 8


def cmul(a, b):
    return (a[0] * b[0] - a[1] * b[1], a[0] * b[1] + a[1] * b[0])


def conj_mul(a, b):
    return (a[0] * b[0] + a[1] * b[1], a[0] * b[1] - a[1] * b[0])


def cadd(a, b):
    return (a[0] + b[0], a[1] + b[1])


def row(x, s):
    return jnp.broadcast_to(x[s : s + 1, :], (SUBS, LANES))


def scan_kernel(trans, drive, back, w, chunk, msg, raw, sems, *, channels, steps):
    portions = LANES // channels
    span = steps // portions
    length = span // SUBS
    pitch = length + 1
    piece = min(length, LANES)
    sources = (trans.at[0], trans.at[2], drive.at[0], drive.at[1], back.at[0], back.at[1])
    copies = [pltpu.make_async_copy(s, raw.at[k], sems.at[k]) for k, s in enumerate(sources)]
    for copy in copies:
        copy.start()
    for k, copy in enumerate(copies):
        copy.wait()
        for g in range(span // LANES):
            x = jnp.concatenate(
                [raw[k, :, pl.ds(q * span + g * LANES, LANES)] for q in range(portions)], axis=0
            )
            xt = x.T
            for first in range(0, LANES, piece):
                r = g * LANES + first
                w[k, pl.ds((r // length) * pitch + r % length, piece), :] = xt[first : first + piece]

    zero = jnp.zeros((SUBS, LANES), jnp.float32)
    one = jnp.ones((SUBS, LANES), jnp.float32)

    def step(i, c):
        p, f, q, g, af, bf, cf, ab, bb, cb = c
        at = lambda k, t: w[k, pl.ds(t, SUBS, stride=pitch), :]
        z = (at(0, i), at(1, i))
        p = cmul(z, p)
        f = cadd(cmul(z, f), (at(2, i), at(3, i)))
        af = af + (f[0] * f[0] + f[1] * f[1])
        bf = cadd(bf, conj_mul(p, f))
        cf = cf + (p[0] * p[0] + p[1] * p[1])
        j = length - 1 - i
        y = (at(0, j), at(1, j))
        q = conj_mul(y, q)
        g = cadd(conj_mul(y, g), (at(4, j), at(5, j)))
        ab = ab + (g[0] * g[0] + g[1] * g[1])
        bb = cadd(bb, conj_mul(q, g))
        cb = cb + (q[0] * q[0] + q[1] * q[1])
        return p, f, q, g, af, bf, cf, ab, bb, cb

    nil = (zero, zero)
    unit = (one, zero)
    p, f, q, g, af, bf, cf, ab, bb, cb = lax.fori_loop(
        0, length, step, (unit, nil, unit, nil, zero, nil, zero, zero, nil, zero), unroll=8
    )

    sub = lax.broadcasted_iota(jnp.int32, (SUBS, LANES), 0)
    portion = lax.broadcasted_iota(jnp.int32, (SUBS, LANES), 1) // channels

    def pick(mask, a, b):
        return tuple(jnp.where(mask, x, y) for x, y in zip(a, b))

    def spread(v):
        total = v
        for m in range(1, portions):
            total = total + pltpu.roll(v, m * channels, 1)
        return total

    def combine(m, v, order, edge, shift):
        start, product = nil, unit
        base_v, base_m = nil, unit
        for s in order:
            base_v = pick(sub == s, start, base_v)
            base_m = pick(sub == s, product, base_m)
            ms, vs = (row(m[0], s), row(m[1], s)), (row(v[0], s), row(v[1], s))
            start = cadd(cmul(ms, start), vs)
            product = cmul(ms, product)
        ex_v, ex_m = nil, unit
        for _ in range(portions - 1):
            nv, nm = cadd(cmul(product, ex_v), start), cmul(product, ex_m)
            nv = tuple(pltpu.roll(a, shift, 1) for a in nv)
            nm = tuple(pltpu.roll(a, shift, 1) for a in nm)
            ex_v, ex_m = pick(portion == edge, nil, nv), pick(portion == edge, unit, nm)
        base_v = cadd(base_v, cmul(base_m, ex_v))
        base_m = cmul(base_m, ex_m)
        total_v, total_m = cadd(cmul(product, ex_v), start), cmul(product, ex_m)
        last = portion == portions - 1 - edge
        total_v = tuple(spread(jnp.where(last, a, zero)) for a in total_v)
        total_m = tuple(spread(jnp.where(last, a, zero)) for a in total_m)
        return base_v, base_m, total_v, total_m

    def stats(a, b, c, v, m):
        cross = conj_mul(v, b)
        whole = a + 2.0 * cross[0] + (v[0] * v[0] + v[1] * v[1]) * c
        mixed = conj_mul(m, (b[0] + c * v[0], b[1] + c * v[1]))
        square = (m[0] * m[0] + m[1] * m[1]) * c
        return tuple(
            spread(jnp.broadcast_to(jnp.sum(x, axis=0, keepdims=True), (SUBS, LANES)))
            for x in (whole, mixed[0], mixed[1], square)
        )

    f0, p0, fe, pe = combine(p, f, range(SUBS), 0, channels)
    g0, q0, ge, _ = combine(
        q, g, range(SUBS - 1, -1, -1), portions - 1, (LANES - channels) % LANES
    )
    for k, x in enumerate(f0 + p0 + g0 + q0):
        chunk[k] = x
    rows = pe + fe + ge + stats(af, bf, cf, f0, p0) + stats(ab, bb, cb, g0, q0)
    for half in range(2):
        block = zero
        for s, x in enumerate(rows[half * SUBS : (half + 1) * SUBS]):
            block = jnp.where(sub == s, x, block)
        msg[half * SUBS : (half + 1) * SUBS, :] = block


def readout_rows(weights, s_ref, out, target, *, channels, steps):
    portions = LANES // channels
    span = steps // portions
    length = span // SUBS
    pitch = length + 1
    piece = min(length, LANES)
    left = jnp.concatenate(
        [
            jnp.concatenate(
                [pltpu.roll(weights[k], q * channels, 1) if q else weights[k] for q in range(portions)],
                axis=0,
            )
            for k in range(2)
        ],
        axis=1,
    )

    def split(x):
        high = x.astype(jnp.bfloat16)
        return high, (x - high.astype(jnp.float32)).astype(jnp.bfloat16)

    def dot(a, b):
        return lax.dot_general(a, b, (((1,), (1,)), ((), ())), preferred_element_type=jnp.float32)

    left_high, left_low = split(left)
    for g in range(span // LANES):
        parts = []
        for k in range(2):
            rows = []
            for first in range(0, LANES, piece):
                r = g * LANES + first
                rows.append(s_ref[k, pl.ds((r // length) * pitch + r % length, piece), :])
            parts.append(jnp.concatenate(rows, axis=0) if len(rows) > 1 else rows[0])
        high, low = split(jnp.concatenate(parts, axis=1))
        res = dot(left_high, high) + (dot(left_high, low) + dot(left_low, high))
        for q in range(portions):
            out[target, :, pl.ds(q * span + g * LANES, LANES)] = res[q * channels : (q + 1) * channels]


def state_kernel(place, gath, chunk, w, weights, out, s_ref, *, channels, steps, devices):
    portions = LANES // channels
    length = steps // portions // SUBS
    pitch = length + 1
    here = place[0]

    def take(j, r):
        return gath[pl.ds(j * 16 + r, 1), :]

    def full(x):
        return jnp.broadcast_to(x, (SUBS, LANES))

    def square(j, base, v):
        cross = conj_mul(v, (take(j, base + 1), take(j, base + 2)))
        return (
            take(j, base) + 2.0 * cross[0] + (v[0] * v[0] + v[1] * v[1]) * take(j, base + 3)
        )

    def walk(j, c):
        f, mine_f, sum_f, g, mine_g, sum_g = c
        sum_f = sum_f + square(j, 6, f)
        mine_f = tuple(jnp.where(j == here, a, b) for a, b in zip(f, mine_f))
        f = cadd(cmul((take(j, 0), take(j, 1)), f), (take(j, 2), take(j, 3)))
        i = devices - 1 - j
        sum_g = sum_g + square(i, 10, g)
        mine_g = tuple(jnp.where(i == here, a, b) for a, b in zip(g, mine_g))
        g = cadd(conj_mul((take(i, 0), take(i, 1)), g), (take(i, 4), take(i, 5)))
        return f, mine_f, sum_f, g, mine_g, sum_g

    last = devices - 1
    f, g = (take(0, 2), take(0, 3)), (take(last, 4), take(last, 5))
    _, f, sum_f, _, g, sum_g = lax.fori_loop(
        1, devices, walk, (f, f, take(0, 6), g, g, take(last, 10)), unroll=5
    )
    f = tuple(jnp.where(here == 0, 0.0, a) for a in f)
    g = tuple(jnp.where(here == last, 0.0, a) for a in g)
    count = 2.0 * steps * devices
    scale_f = full(1.0 / jnp.sqrt(sum_f / count + epsilon))
    scale_g = full(1.0 / jnp.sqrt(sum_g / count + epsilon))
    f, g = tuple(map(full, f)), tuple(map(full, g))
    f = cadd((chunk[0], chunk[1]), cmul((chunk[2], chunk[3]), f))
    g = cadd((chunk[4], chunk[5]), cmul((chunk[6], chunk[7]), g))
    half = length // 2

    def step(i, c, later):
        f, g = c
        at = lambda k, t: w[k, pl.ds(t, SUBS, stride=pitch), :]
        j = length - 1 - i
        f = cadd(cmul((at(0, i), at(1, i)), f), (at(2, i), at(3, i)))
        g = cadd(conj_mul((at(0, j), at(1, j)), g), (at(4, j), at(5, j)))
        for k in range(2):
            a = f[k] * scale_f
            b = g[k] * scale_g
            if later:
                a = a + s_ref[k, pl.ds(i, SUBS, stride=pitch), :]
                b = b + s_ref[k, pl.ds(j, SUBS, stride=pitch), :]
            s_ref[k, pl.ds(i, SUBS, stride=pitch), :] = a
            s_ref[k, pl.ds(j, SUBS, stride=pitch), :] = b
        return f, g

    c = lax.fori_loop(0, half, lambda i, c: step(i, c, False), (f, g), unroll=8)
    lax.fori_loop(half, length, lambda i, c: step(i, c, True), c, unroll=8)
    for t in range(weights.shape[0]):
        readout_rows(weights.at[t], s_ref, out, t, channels=channels, steps=steps)


def own_kernel(weights, s_ref, out, *, channels, steps):
    readout_rows(weights.at[0], s_ref, out, 0, channels=channels, steps=steps)


VM = pl.BlockSpec(memory_space=pltpu.VMEM)
PARAMS = pltpu.CompilerParams(vmem_limit_bytes=40 * 1024 * 1024)


def on_device(trans, drive, back_drive, readout):
    channels = trans.shape[1]
    steps = trans.shape[2]
    devices = lax.axis_size("tm")
    groups = lax.axis_size("chan")
    portions = LANES // channels
    length = steps // portions // SUBS
    rows = SUBS * (length + 1)
    rows = (rows + 7) // 8 * 8
    here = lax.axis_index("chan")
    f32 = jnp.float32

    by_part = jnp.moveaxis(readout, 1, 0)

    def weights_for(other):
        mine = lax.dynamic_slice_in_dim(by_part, other * channels, channels, 2)
        return jnp.pad(mine, ((0, 0), (0, 0), (0, LANES - channels)))

    others = []
    for k in range(1, groups):
        pairs = [(j, (j + k) % groups) for j in range(groups)]
        others.append(lax.ppermute(weights_for((here + k) % groups), "chan", pairs))

    any_spec = pl.BlockSpec(memory_space=pltpu.HBM)
    w, chunk, msg = pl.pallas_call(
        lambda *refs: scan_kernel(*refs, channels=channels, steps=steps),
        out_shape=(
            jax.ShapeDtypeStruct((6, rows, LANES), f32),
            jax.ShapeDtypeStruct((8, SUBS, LANES), f32),
            jax.ShapeDtypeStruct((16, LANES), f32),
        ),
        in_specs=[any_spec] * 3,
        out_specs=(VM, VM, VM),
        scratch_shapes=[pltpu.VMEM((6, channels, steps), f32), pltpu.SemaphoreType.DMA((6,))],
        compiler_params=PARAMS,
        name="local_scan",
    )(trans, drive, back_drive)
    gathered = lax.all_gather(msg, "tm", axis=0, tiled=True)
    place = lax.axis_index("tm").reshape(1).astype(jnp.int32)
    out, states = pl.pallas_call(
        lambda *refs: state_kernel(*refs, channels=channels, steps=steps, devices=devices),
        out_shape=(
            jax.ShapeDtypeStruct((groups - 1, channels, steps), f32),
            jax.ShapeDtypeStruct((2, rows, LANES), f32),
        ),
        in_specs=[pl.BlockSpec(memory_space=pltpu.SMEM), VM, VM, VM, VM],
        out_specs=(VM, VM),
        compiler_params=PARAMS,
        name="states",
    )(place, gathered, chunk, w, jnp.stack(others))
    received = []
    for k in range(1, groups):
        pairs = [(j, (j - k) % groups) for j in range(groups)]
        received.append(lax.ppermute(out[k - 1], "chan", pairs))
    own = pl.pallas_call(
        lambda *refs: own_kernel(*refs, channels=channels, steps=steps),
        out_shape=jax.ShapeDtypeStruct((1, channels, steps), f32),
        in_specs=[VM, VM],
        out_specs=VM,
        compiler_params=PARAMS,
        cost_estimate=pl.CostEstimate(
            flops=12 * LANES * LANES * steps, bytes_accessed=4 * channels * steps, transcendentals=0
        ),
        name="own",
    )(weights_for(here)[None], states)[0]
    for part in received:
        own = own + part
    return own


def solution(mesh):
    in_specs = (
        P(None, "chan", "tm"),
        P(None, "chan", "tm"),
        P(None, "chan", "tm"),
        P("chan", None, None),
    )
    out_specs = P("chan", "tm")
    return jax.shard_map(
        on_device, mesh=mesh, in_specs=in_specs, out_specs=out_specs, check_vma=False
    )
```

```python
import jax
import jax.numpy as jnp
from jax import lax
from jax.experimental import pallas as pl
from jax.experimental.pallas import tpu as pltpu
from jax.sharding import PartitionSpec as P

epsilon = 1e-06
LANES = 128
SUBS = 8


def cmul(a, b):
    return (a[0] * b[0] - a[1] * b[1], a[0] * b[1] + a[1] * b[0])


def conj_mul(a, b):
    return (a[0] * b[0] + a[1] * b[1], a[0] * b[1] - a[1] * b[0])


def cadd(a, b):
    return (a[0] + b[0], a[1] + b[1])


def row(x, s):
    return jnp.broadcast_to(x[s : s + 1, :], (SUBS, LANES))


def digits(devices):
    found = []
    while devices > 1:
        base = 4 if devices % 4 == 0 else 2 if devices % 2 == 0 else devices
        found.append(base)
        devices //= base
    return found


def slot_of(j, here, devices):
    slot, stride = 0, 1
    for base in digits(devices):
        slot = slot + stride * ((here // stride % base - j // stride % base + base) % base)
        stride *= base
    return slot


def gather_stages(msg, devices):
    parts, stride = [msg], 1
    for base in digits(devices):
        buf = jnp.concatenate(parts, axis=0) if len(parts) > 1 else parts[0]
        parts = [buf]
        for k in range(1, base):
            pairs = []
            for j in range(devices):
                d = j // stride % base
                pairs.append((j, j + ((d + k) % base - d) * stride))
            parts.append(lax.ppermute(buf, "tm", pairs))
        stride *= base
    return parts


def scan_kernel(
    side, trans, drive, back, readout, w, chunk, msg, weights, raw, table, sems, *, channels, steps
):
    portions = LANES // channels
    span = steps // portions
    length = span // SUBS
    pitch = length + 1
    piece = min(length, LANES)
    sources = (trans.at[0], trans.at[2], drive.at[0], drive.at[1], back.at[0], back.at[1])
    copies = [pltpu.make_async_copy(s, raw.at[k], sems.at[k]) for k, s in enumerate(sources)]
    copies.append(pltpu.make_async_copy(readout, table, sems.at[len(sources)]))
    for copy in copies:
        copy.start()
    for k, copy in enumerate(copies[:-1]):
        copy.wait()
        for g in range(span // LANES):
            x = jnp.concatenate(
                [raw[k, :, pl.ds(q * span + g * LANES, LANES)] for q in range(portions)], axis=0
            )
            xt = x.T
            for first in range(0, LANES, piece):
                r = g * LANES + first
                w[k, pl.ds((r // length) * pitch + r % length, piece), :] = xt[first : first + piece]

    copies[-1].wait()
    low = lax.broadcasted_iota(jnp.int32, (channels, LANES), 1) < channels
    for t in range(weights.shape[0]):
        other = (side[0] + t) % weights.shape[0]
        for k in range(2):
            shifted = pltpu.roll(table[:, k, :], (LANES - other * channels) % LANES, 1)
            weights[t, k] = jnp.where(low, shifted, 0.0)

    zero = jnp.zeros((SUBS, LANES), jnp.float32)
    one = jnp.ones((SUBS, LANES), jnp.float32)

    def step(i, c):
        p, f, q, g, af, bf, cf, ab, bb, cb = c
        at = lambda k, t: w[k, pl.ds(t, SUBS, stride=pitch), :]
        z = (at(0, i), at(1, i))
        p = cmul(z, p)
        f = cadd(cmul(z, f), (at(2, i), at(3, i)))
        af = af + (f[0] * f[0] + f[1] * f[1])
        bf = cadd(bf, conj_mul(p, f))
        cf = cf + (p[0] * p[0] + p[1] * p[1])
        j = length - 1 - i
        y = (at(0, j), at(1, j))
        q = conj_mul(y, q)
        g = cadd(conj_mul(y, g), (at(4, j), at(5, j)))
        ab = ab + (g[0] * g[0] + g[1] * g[1])
        bb = cadd(bb, conj_mul(q, g))
        cb = cb + (q[0] * q[0] + q[1] * q[1])
        return p, f, q, g, af, bf, cf, ab, bb, cb

    nil = (zero, zero)
    unit = (one, zero)
    p, f, q, g, af, bf, cf, ab, bb, cb = lax.fori_loop(
        0, length, step, (unit, nil, unit, nil, zero, nil, zero, zero, nil, zero), unroll=8
    )

    sub = lax.broadcasted_iota(jnp.int32, (SUBS, LANES), 0)
    portion = lax.broadcasted_iota(jnp.int32, (SUBS, LANES), 1) // channels

    def pick(mask, a, b):
        return tuple(jnp.where(mask, x, y) for x, y in zip(a, b))

    def spread(v):
        total = v
        for m in range(1, portions):
            total = total + pltpu.roll(v, m * channels, 1)
        return total

    def combine(m, v, order, edge, shift):
        start, product = nil, unit
        base_v, base_m = nil, unit
        for s in order:
            base_v = pick(sub == s, start, base_v)
            base_m = pick(sub == s, product, base_m)
            ms, vs = (row(m[0], s), row(m[1], s)), (row(v[0], s), row(v[1], s))
            start = cadd(cmul(ms, start), vs)
            product = cmul(ms, product)
        ex_v, ex_m = nil, unit
        for _ in range(portions - 1):
            nv, nm = cadd(cmul(product, ex_v), start), cmul(product, ex_m)
            nv = tuple(pltpu.roll(a, shift, 1) for a in nv)
            nm = tuple(pltpu.roll(a, shift, 1) for a in nm)
            ex_v, ex_m = pick(portion == edge, nil, nv), pick(portion == edge, unit, nm)
        base_v = cadd(base_v, cmul(base_m, ex_v))
        base_m = cmul(base_m, ex_m)
        total_v, total_m = cadd(cmul(product, ex_v), start), cmul(product, ex_m)
        last = portion == portions - 1 - edge
        total_v = tuple(spread(jnp.where(last, a, zero)) for a in total_v)
        total_m = tuple(spread(jnp.where(last, a, zero)) for a in total_m)
        return base_v, base_m, total_v, total_m

    def stats(a, b, c, v, m):
        cross = conj_mul(v, b)
        whole = a + 2.0 * cross[0] + (v[0] * v[0] + v[1] * v[1]) * c
        mixed = conj_mul(m, (b[0] + c * v[0], b[1] + c * v[1]))
        square = (m[0] * m[0] + m[1] * m[1]) * c
        return tuple(
            spread(jnp.broadcast_to(jnp.sum(x, axis=0, keepdims=True), (SUBS, LANES)))
            for x in (whole, mixed[0], mixed[1], square)
        )

    f0, p0, fe, pe = combine(p, f, range(SUBS), 0, channels)
    g0, q0, ge, _ = combine(
        q, g, range(SUBS - 1, -1, -1), portions - 1, (LANES - channels) % LANES
    )
    for k, x in enumerate(f0 + p0 + g0 + q0):
        chunk[k] = x
    rows = pe + fe + ge + stats(af, bf, cf, f0, p0) + stats(ab, bb, cb, g0, q0)
    for half in range(2):
        block = zero
        for s, x in enumerate(rows[half * SUBS : (half + 1) * SUBS]):
            block = jnp.where(sub == s, x, block)
        msg[half * SUBS : (half + 1) * SUBS, :] = block


def readout_rows(weights, s_ref, out, target, *, channels, steps):
    portions = LANES // channels
    span = steps // portions
    length = span // SUBS
    pitch = length + 1
    piece = min(length, LANES)
    left = jnp.concatenate(
        [
            jnp.concatenate(
                [pltpu.roll(weights[k], q * channels, 1) if q else weights[k] for q in range(portions)],
                axis=0,
            )
            for k in range(2)
        ],
        axis=1,
    )

    def split(x):
        high = x.astype(jnp.bfloat16)
        return high, (x - high.astype(jnp.float32)).astype(jnp.bfloat16)

    def dot(a, b):
        return lax.dot_general(a, b, (((1,), (1,)), ((), ())), preferred_element_type=jnp.float32)

    left_high, left_low = split(left)
    for g in range(span // LANES):
        parts = []
        for k in range(2):
            rows = []
            for first in range(0, LANES, piece):
                r = g * LANES + first
                rows.append(s_ref[k, pl.ds((r // length) * pitch + r % length, piece), :])
            parts.append(jnp.concatenate(rows, axis=0) if len(rows) > 1 else rows[0])
        high, low = split(jnp.concatenate(parts, axis=1))
        res = dot(left_high, high) + (dot(left_high, low) + dot(left_low, high))
        for q in range(portions):
            out[target, :, pl.ds(q * span + g * LANES, LANES)] = res[q * channels : (q + 1) * channels]


def state_kernel(place, chunk, w, *rest, channels, steps, devices):
    parts, weights, (out, s_ref, gath) = rest[:-4], rest[-4], rest[-3:]
    for k, part in enumerate(parts):
        size = part.shape[0]
        gath[k * size : (k + 1) * size, :] = part[...]
    portions = LANES // channels
    length = steps // portions // SUBS
    pitch = length + 1
    here = place[0]

    def take(j, r):
        return gath[pl.ds(slot_of(j, here, devices) * 16 + r, 1), :]

    def full(x):
        return jnp.broadcast_to(x, (SUBS, LANES))

    def square(j, base, v):
        cross = conj_mul(v, (take(j, base + 1), take(j, base + 2)))
        return (
            take(j, base) + 2.0 * cross[0] + (v[0] * v[0] + v[1] * v[1]) * take(j, base + 3)
        )

    def walk(j, c):
        f, mine_f, sum_f, g, mine_g, sum_g = c
        sum_f = sum_f + square(j, 6, f)
        mine_f = tuple(jnp.where(j == here, a, b) for a, b in zip(f, mine_f))
        f = cadd(cmul((take(j, 0), take(j, 1)), f), (take(j, 2), take(j, 3)))
        i = devices - 1 - j
        sum_g = sum_g + square(i, 10, g)
        mine_g = tuple(jnp.where(i == here, a, b) for a, b in zip(g, mine_g))
        g = cadd(conj_mul((take(i, 0), take(i, 1)), g), (take(i, 4), take(i, 5)))
        return f, mine_f, sum_f, g, mine_g, sum_g

    last = devices - 1
    f, g = (take(0, 2), take(0, 3)), (take(last, 4), take(last, 5))
    _, f, sum_f, _, g, sum_g = lax.fori_loop(
        1, devices, walk, (f, f, take(0, 6), g, g, take(last, 10)), unroll=5
    )
    f = tuple(jnp.where(here == 0, 0.0, a) for a in f)
    g = tuple(jnp.where(here == last, 0.0, a) for a in g)
    count = 2.0 * steps * devices
    scale_f = full(1.0 / jnp.sqrt(sum_f / count + epsilon))
    scale_g = full(1.0 / jnp.sqrt(sum_g / count + epsilon))
    f, g = tuple(map(full, f)), tuple(map(full, g))
    f = cadd((chunk[0], chunk[1]), cmul((chunk[2], chunk[3]), f))
    g = cadd((chunk[4], chunk[5]), cmul((chunk[6], chunk[7]), g))
    half = length // 2

    def step(i, c, later):
        f, g = c
        at = lambda k, t: w[k, pl.ds(t, SUBS, stride=pitch), :]
        j = length - 1 - i
        f = cadd(cmul((at(0, i), at(1, i)), f), (at(2, i), at(3, i)))
        g = cadd(conj_mul((at(0, j), at(1, j)), g), (at(4, j), at(5, j)))
        for k in range(2):
            a = f[k] * scale_f
            b = g[k] * scale_g
            if later:
                a = a + s_ref[k, pl.ds(i, SUBS, stride=pitch), :]
                b = b + s_ref[k, pl.ds(j, SUBS, stride=pitch), :]
            s_ref[k, pl.ds(i, SUBS, stride=pitch), :] = a
            s_ref[k, pl.ds(j, SUBS, stride=pitch), :] = b
        return f, g

    c = lax.fori_loop(0, half, lambda i, c: step(i, c, False), (f, g), unroll=8)
    lax.fori_loop(half, length, lambda i, c: step(i, c, True), c, unroll=8)
    for t in range(weights.shape[0]):
        readout_rows(weights.at[t], s_ref, out, t, channels=channels, steps=steps)


def own_kernel(weights, s_ref, out, *, channels, steps):
    readout_rows(weights.at[0], s_ref, out, 0, channels=channels, steps=steps)


VM = pl.BlockSpec(memory_space=pltpu.VMEM)
PARAMS = pltpu.CompilerParams(vmem_limit_bytes=40 * 1024 * 1024)


def on_device(trans, drive, back_drive, readout):
    channels = trans.shape[1]
    steps = trans.shape[2]
    devices = lax.axis_size("tm")
    groups = lax.axis_size("chan")
    portions = LANES // channels
    length = steps // portions // SUBS
    rows = SUBS * (length + 1)
    rows = (rows + 7) // 8 * 8
    here = lax.axis_index("chan")
    f32 = jnp.float32

    hbm_spec = pl.BlockSpec(memory_space=pltpu.HBM)
    smem_spec = pl.BlockSpec(memory_space=pltpu.SMEM)
    trans, drive, back_drive, readout = (
        pltpu.with_memory_space_constraint(x, pltpu.HBM)
        for x in (trans, drive, back_drive, readout)
    )
    w, chunk, msg, weights = pl.pallas_call(
        lambda *refs: scan_kernel(*refs, channels=channels, steps=steps),
        out_shape=(
            jax.ShapeDtypeStruct((6, rows, LANES), f32),
            jax.ShapeDtypeStruct((8, SUBS, LANES), f32),
            jax.ShapeDtypeStruct((16, LANES), f32),
            jax.ShapeDtypeStruct((groups, 2, channels, LANES), f32),
        ),
        in_specs=[smem_spec] + [hbm_spec] * 4,
        out_specs=(VM, VM, VM, VM),
        scratch_shapes=[
            pltpu.VMEM((6, channels, steps), f32),
            pltpu.VMEM(readout.shape, f32),
            pltpu.SemaphoreType.DMA((7,)),
        ],
        compiler_params=PARAMS,
        name="local_scan",
    )(here.reshape(1).astype(jnp.int32), trans, drive, back_drive, readout)
    parts = gather_stages(msg, devices)
    others = []
    for k in range(1, groups):
        pairs = [(j, (j + k) % groups) for j in range(groups)]
        others.append(lax.ppermute(weights[k], "chan", pairs))
    place = lax.axis_index("tm").reshape(1).astype(jnp.int32)
    out, states = pl.pallas_call(
        lambda *refs: state_kernel(*refs, channels=channels, steps=steps, devices=devices),
        out_shape=(
            jax.ShapeDtypeStruct((groups - 1, channels, steps), f32),
            jax.ShapeDtypeStruct((2, rows, LANES), f32),
        ),
        in_specs=[smem_spec] + [VM] * (3 + len(parts)),
        out_specs=(VM, VM),
        scratch_shapes=[pltpu.VMEM((16 * devices, LANES), f32)],
        compiler_params=PARAMS,
        name="states",
    )(place, chunk, w, *parts, jnp.stack(others))
    received = []
    for k in range(1, groups):
        pairs = [(j, (j - k) % groups) for j in range(groups)]
        received.append(lax.ppermute(out[k - 1], "chan", pairs))
    own = pl.pallas_call(
        lambda *refs: own_kernel(*refs, channels=channels, steps=steps),
        out_shape=jax.ShapeDtypeStruct((1, channels, steps), f32),
        in_specs=[VM, VM],
        out_specs=VM,
        compiler_params=PARAMS,
        cost_estimate=pl.CostEstimate(
            flops=12 * LANES * LANES * steps, bytes_accessed=4 * channels * steps, transcendentals=0
        ),
        name="own",
    )(weights[:1], states)[0]
    for part in received:
        own = own + part
    return own


def solution(mesh):
    in_specs = (
        P(None, "chan", "tm"),
        P(None, "chan", "tm"),
        P(None, "chan", "tm"),
        P("chan", None, None),
    )
    out_specs = P("chan", "tm")
    return jax.shard_map(
        on_device, mesh=mesh, in_specs=in_specs, out_specs=out_specs, check_vma=False
    )
```

```python
import jax
import jax.numpy as jnp
from jax import lax
from jax.experimental import pallas as pl
from jax.experimental.pallas import tpu as pltpu
from jax.sharding import PartitionSpec as P

epsilon = 1e-06
LANES = 128
SUBS = 8


def cmul(a, b):
    return (a[0] * b[0] - a[1] * b[1], a[0] * b[1] + a[1] * b[0])


def conj_mul(a, b):
    return (a[0] * b[0] + a[1] * b[1], a[0] * b[1] - a[1] * b[0])


def cadd(a, b):
    return (a[0] + b[0], a[1] + b[1])


def row(x, s):
    return jnp.broadcast_to(x[s : s + 1, :], (SUBS, LANES))


def digits(devices):
    found = []
    while devices > 1:
        base = 4 if devices % 4 == 0 else 2 if devices % 2 == 0 else devices
        found.append(base)
        devices //= base
    return found


def slot_of(j, here, devices):
    slot, stride = 0, 1
    for base in digits(devices):
        if base & (base - 1):
            away = (here // stride % base - j // stride % base + base) % base
        else:
            shift = stride.bit_length() - 1
            away = ((here >> shift) - (j >> shift)) & (base - 1)
        slot = slot + stride * away
        stride *= base
    return slot


def gather_stages(msg, devices):
    parts, stride = [msg], 1
    for base in digits(devices):
        buf = jnp.concatenate(parts, axis=0) if len(parts) > 1 else parts[0]
        parts = [buf]
        for k in range(1, base):
            pairs = []
            for j in range(devices):
                d = j // stride % base
                pairs.append((j, j + ((d + k) % base - d) * stride))
            parts.append(lax.ppermute(buf, "tm", pairs))
        stride *= base
    return parts


def scan_kernel(
    side, trans, drive, back, readout, w, chunk, msg, weights, raw, table, sems, *, channels, steps
):
    portions = LANES // channels
    span = steps // portions
    length = span // SUBS
    pitch = length + 1
    piece = min(length, LANES)
    sources = (trans.at[0], trans.at[2], drive.at[0], drive.at[1], back.at[0], back.at[1])
    copies = [pltpu.make_async_copy(s, raw.at[k], sems.at[k]) for k, s in enumerate(sources)]
    copies.append(pltpu.make_async_copy(readout, table, sems.at[len(sources)]))
    for copy in copies:
        copy.start()
    for k, copy in enumerate(copies[:-1]):
        copy.wait()
        for g in range(span // LANES):
            x = jnp.concatenate(
                [raw[k, :, pl.ds(q * span + g * LANES, LANES)] for q in range(portions)], axis=0
            )
            xt = x.T
            for first in range(0, LANES, piece):
                r = g * LANES + first
                w[k, pl.ds((r // length) * pitch + r % length, piece), :] = xt[first : first + piece]

    copies[-1].wait()
    low = lax.broadcasted_iota(jnp.int32, (channels, LANES), 1) < channels
    for t in range(weights.shape[0]):
        other = (side[0] + t) % weights.shape[0]
        for k in range(2):
            shifted = pltpu.roll(table[:, k, :], (LANES - other * channels) % LANES, 1)
            weights[t, k] = jnp.where(low, shifted, 0.0)

    zero = jnp.zeros((SUBS, LANES), jnp.float32)
    one = jnp.ones((SUBS, LANES), jnp.float32)

    def step(i, c):
        p, f, q, g, af, bf, cf, ab, bb, cb = c
        at = lambda k, t: w[k, pl.ds(t, SUBS, stride=pitch), :]
        z = (at(0, i), at(1, i))
        p = cmul(z, p)
        f = cadd(cmul(z, f), (at(2, i), at(3, i)))
        af = af + (f[0] * f[0] + f[1] * f[1])
        bf = cadd(bf, conj_mul(p, f))
        cf = cf + (p[0] * p[0] + p[1] * p[1])
        j = length - 1 - i
        y = (at(0, j), at(1, j))
        q = conj_mul(y, q)
        g = cadd(conj_mul(y, g), (at(4, j), at(5, j)))
        ab = ab + (g[0] * g[0] + g[1] * g[1])
        bb = cadd(bb, conj_mul(q, g))
        cb = cb + (q[0] * q[0] + q[1] * q[1])
        return p, f, q, g, af, bf, cf, ab, bb, cb

    nil = (zero, zero)
    unit = (one, zero)
    p, f, q, g, af, bf, cf, ab, bb, cb = lax.fori_loop(
        0, length, step, (unit, nil, unit, nil, zero, nil, zero, zero, nil, zero), unroll=8
    )

    sub = lax.broadcasted_iota(jnp.int32, (SUBS, LANES), 0)
    portion = lax.broadcasted_iota(jnp.int32, (SUBS, LANES), 1) // channels

    def pick(mask, a, b):
        return tuple(jnp.where(mask, x, y) for x, y in zip(a, b))

    def spread(v):
        total = v
        for m in range(1, portions):
            total = total + pltpu.roll(v, m * channels, 1)
        return total

    def combine(m, v, order, edge, shift):
        start, product = nil, unit
        base_v, base_m = nil, unit
        for s in order:
            base_v = pick(sub == s, start, base_v)
            base_m = pick(sub == s, product, base_m)
            ms, vs = (row(m[0], s), row(m[1], s)), (row(v[0], s), row(v[1], s))
            start = cadd(cmul(ms, start), vs)
            product = cmul(ms, product)
        ex_v, ex_m = nil, unit
        for _ in range(portions - 1):
            nv, nm = cadd(cmul(product, ex_v), start), cmul(product, ex_m)
            nv = tuple(pltpu.roll(a, shift, 1) for a in nv)
            nm = tuple(pltpu.roll(a, shift, 1) for a in nm)
            ex_v, ex_m = pick(portion == edge, nil, nv), pick(portion == edge, unit, nm)
        base_v = cadd(base_v, cmul(base_m, ex_v))
        base_m = cmul(base_m, ex_m)
        total_v, total_m = cadd(cmul(product, ex_v), start), cmul(product, ex_m)
        last = portion == portions - 1 - edge
        total_v = tuple(spread(jnp.where(last, a, zero)) for a in total_v)
        total_m = tuple(spread(jnp.where(last, a, zero)) for a in total_m)
        return base_v, base_m, total_v, total_m

    def stats(a, b, c, v, m):
        cross = conj_mul(v, b)
        whole = a + 2.0 * cross[0] + (v[0] * v[0] + v[1] * v[1]) * c
        mixed = conj_mul(m, (b[0] + c * v[0], b[1] + c * v[1]))
        square = (m[0] * m[0] + m[1] * m[1]) * c
        return tuple(
            spread(jnp.broadcast_to(jnp.sum(x, axis=0, keepdims=True), (SUBS, LANES)))
            for x in (whole, mixed[0], mixed[1], square)
        )

    f0, p0, fe, pe = combine(p, f, range(SUBS), 0, channels)
    g0, q0, ge, _ = combine(
        q, g, range(SUBS - 1, -1, -1), portions - 1, (LANES - channels) % LANES
    )
    for k, x in enumerate(f0 + p0 + g0 + q0):
        chunk[k] = x
    rows = pe + fe + ge + stats(af, bf, cf, f0, p0) + stats(ab, bb, cb, g0, q0)
    for half in range(2):
        block = zero
        for s, x in enumerate(rows[half * SUBS : (half + 1) * SUBS]):
            block = jnp.where(sub == s, x, block)
        msg[half * SUBS : (half + 1) * SUBS, :] = block


def readout_rows(weights, s_ref, out, target, groups, *, channels, steps):
    portions = LANES // channels
    span = steps // portions
    length = span // SUBS
    pitch = length + 1
    piece = min(length, LANES)
    left = jnp.concatenate(
        [
            jnp.concatenate(
                [pltpu.roll(weights[k], q * channels, 1) if q else weights[k] for q in range(portions)],
                axis=0,
            )
            for k in range(2)
        ],
        axis=1,
    )

    def split(x):
        high = x.astype(jnp.bfloat16)
        return high, (x - high.astype(jnp.float32)).astype(jnp.bfloat16)

    def dot(a, b):
        return lax.dot_general(a, b, (((1,), (1,)), ((), ())), preferred_element_type=jnp.float32)

    left_high, left_low = split(left)
    width = len(groups) * LANES
    for g in groups:
        parts = []
        for k in range(2):
            rows = []
            for first in range(0, LANES, piece):
                r = g * LANES + first
                rows.append(s_ref[k, pl.ds((r // length) * pitch + r % length, piece), :])
            parts.append(jnp.concatenate(rows, axis=0) if len(rows) > 1 else rows[0])
        high, low = split(jnp.concatenate(parts, axis=1))
        res = dot(left_high, high) + (dot(left_high, low) + dot(left_low, high))
        for q in range(portions):
            column = q * width + (g - groups[0]) * LANES
            out[target, :, pl.ds(column, LANES)] = res[q * channels : (q + 1) * channels]


def state_kernel(place, chunk, w, *rest, groups, channels, steps, devices):
    parts, weights, (out, s_ref, gath) = rest[:-4], rest[-4], rest[-3:]
    for k, part in enumerate(parts):
        size = part.shape[0]
        gath[k * size : (k + 1) * size, :] = part[...]
    portions = LANES // channels
    length = steps // portions // SUBS
    pitch = length + 1
    here = place[0]

    def take(j, r):
        return gath[pl.ds(slot_of(j, here, devices) * 16 + r, 1), :]

    def full(x):
        return jnp.broadcast_to(x, (SUBS, LANES))

    def square(j, base, v):
        cross = conj_mul(v, (take(j, base + 1), take(j, base + 2)))
        return (
            take(j, base) + 2.0 * cross[0] + (v[0] * v[0] + v[1] * v[1]) * take(j, base + 3)
        )

    def walk(j, c):
        f, mine_f, sum_f, g, mine_g, sum_g = c
        sum_f = sum_f + square(j, 6, f)
        mine_f = tuple(jnp.where(j == here, a, b) for a, b in zip(f, mine_f))
        f = cadd(cmul((take(j, 0), take(j, 1)), f), (take(j, 2), take(j, 3)))
        i = devices - 1 - j
        sum_g = sum_g + square(i, 10, g)
        mine_g = tuple(jnp.where(i == here, a, b) for a, b in zip(g, mine_g))
        g = cadd(conj_mul((take(i, 0), take(i, 1)), g), (take(i, 4), take(i, 5)))
        return f, mine_f, sum_f, g, mine_g, sum_g

    last = devices - 1
    f, g = (take(0, 2), take(0, 3)), (take(last, 4), take(last, 5))
    _, f, sum_f, _, g, sum_g = lax.fori_loop(
        1, devices, walk, (f, f, take(0, 6), g, g, take(last, 10)), unroll=5
    )
    f = tuple(jnp.where(here == 0, 0.0, a) for a in f)
    g = tuple(jnp.where(here == last, 0.0, a) for a in g)
    count = 2.0 * steps * devices
    scale_f = full(1.0 / jnp.sqrt(sum_f / count + epsilon))
    scale_g = full(1.0 / jnp.sqrt(sum_g / count + epsilon))
    f, g = tuple(map(full, f)), tuple(map(full, g))
    f = cadd((chunk[0], chunk[1]), cmul((chunk[2], chunk[3]), f))
    g = cadd((chunk[4], chunk[5]), cmul((chunk[6], chunk[7]), g))
    half = length // 2

    def step(i, c, later):
        f, g = c
        at = lambda k, t: w[k, pl.ds(t, SUBS, stride=pitch), :]
        j = length - 1 - i
        f = cadd(cmul((at(0, i), at(1, i)), f), (at(2, i), at(3, i)))
        g = cadd(conj_mul((at(0, j), at(1, j)), g), (at(4, j), at(5, j)))
        for k in range(2):
            a = f[k] * scale_f
            b = g[k] * scale_g
            if later:
                a = a + s_ref[k, pl.ds(i, SUBS, stride=pitch), :]
                b = b + s_ref[k, pl.ds(j, SUBS, stride=pitch), :]
            s_ref[k, pl.ds(i, SUBS, stride=pitch), :] = a
            s_ref[k, pl.ds(j, SUBS, stride=pitch), :] = b
        return f, g

    c = lax.fori_loop(0, half, lambda i, c: step(i, c, False), (f, g), unroll=8)
    lax.fori_loop(half, length, lambda i, c: step(i, c, True), c, unroll=8)
    for t in range(weights.shape[0]):
        readout_rows(weights.at[t], s_ref, out, t, groups, channels=channels, steps=steps)


def rest_kernel(weights, others, s_ref, out, own, *, groups, channels, steps):
    for t in range(others.shape[0]):
        readout_rows(others.at[t], s_ref, out, t, groups, channels=channels, steps=steps)
    every = range(groups[-1] + 1)
    readout_rows(weights.at[0], s_ref, own, 0, every, channels=channels, steps=steps)


def finish_kernel(*refs, groups, channels, steps, fresh):
    own, *received, out, total, sems = refs if fresh else refs[1:]
    portions = LANES // channels
    span = steps // portions
    width = len(groups) * LANES
    copies = []
    for q in range(portions):
        there = pl.ds(q * span + groups[0] * LANES, width)
        here = pl.ds(q * width, width)
        value = own[0, :, there]
        for part in received:
            value = value + part[:, here]
        total[:, here] = value
        copies.append(pltpu.make_async_copy(total.at[:, here], out.at[:, there], sems.at[q]))
        copies[-1].start()
    for copy in copies:
        copy.wait()


VM = pl.BlockSpec(memory_space=pltpu.VMEM)
PARAMS = pltpu.CompilerParams(vmem_limit_bytes=40 * 1024 * 1024)


def on_device(trans, drive, back_drive, readout):
    channels = trans.shape[1]
    steps = trans.shape[2]
    devices = lax.axis_size("tm")
    groups = lax.axis_size("chan")
    portions = LANES // channels
    length = steps // portions // SUBS
    rows = SUBS * (length + 1)
    rows = (rows + 7) // 8 * 8
    here = lax.axis_index("chan")
    f32 = jnp.float32

    hbm_spec = pl.BlockSpec(memory_space=pltpu.HBM)
    smem_spec = pl.BlockSpec(memory_space=pltpu.SMEM)
    trans, drive, back_drive, readout = (
        pltpu.with_memory_space_constraint(x, pltpu.HBM)
        for x in (trans, drive, back_drive, readout)
    )
    w, chunk, msg, weights = pl.pallas_call(
        lambda *refs: scan_kernel(*refs, channels=channels, steps=steps),
        out_shape=(
            jax.ShapeDtypeStruct((6, rows, LANES), f32),
            jax.ShapeDtypeStruct((8, SUBS, LANES), f32),
            jax.ShapeDtypeStruct((16, LANES), f32),
            jax.ShapeDtypeStruct((groups, 2, channels, LANES), f32),
        ),
        in_specs=[smem_spec] + [hbm_spec] * 4,
        out_specs=(VM, VM, VM, VM),
        scratch_shapes=[
            pltpu.VMEM((6, channels, steps), f32),
            pltpu.VMEM(readout.shape, f32),
            pltpu.SemaphoreType.DMA((7,)),
        ],
        compiler_params=PARAMS,
        name="local_scan",
    )(here.reshape(1).astype(jnp.int32), trans, drive, back_drive, readout)
    parts = gather_stages(msg, devices)
    others = []
    for k in range(1, groups):
        pairs = [(j, (j + k) % groups) for j in range(groups)]
        others.append(lax.ppermute(weights[k], "chan", pairs))
    place = lax.axis_index("tm").reshape(1).astype(jnp.int32)
    pieces = steps // portions // LANES
    tail = max(1, pieces // 4)
    early, late = range(pieces - tail), range(pieces - tail, pieces)
    size = lambda some: len(some) * LANES * portions
    others = jnp.stack(others)
    out, states = pl.pallas_call(
        lambda *refs: state_kernel(
            *refs, groups=early, channels=channels, steps=steps, devices=devices
        ),
        out_shape=(
            jax.ShapeDtypeStruct((groups - 1, channels, size(early)), f32),
            jax.ShapeDtypeStruct((2, rows, LANES), f32),
        ),
        in_specs=[smem_spec] + [VM] * (3 + len(parts)),
        out_specs=(VM, VM),
        scratch_shapes=[pltpu.VMEM((16 * devices, LANES), f32)],
        compiler_params=PARAMS,
        name="states",
    )(place, chunk, w, *parts, others)

    def send(values):
        received = []
        for k in range(1, groups):
            pairs = [(j, (j - k) % groups) for j in range(groups)]
            received.append(lax.ppermute(values[k - 1], "chan", pairs))
        return received

    first = send(out)
    out, own = pl.pallas_call(
        lambda *refs: rest_kernel(*refs, groups=late, channels=channels, steps=steps),
        out_shape=(
            jax.ShapeDtypeStruct((groups - 1, channels, size(late)), f32),
            jax.ShapeDtypeStruct((1, channels, steps), f32),
        ),
        in_specs=[VM, VM, VM],
        out_specs=(VM, VM),
        compiler_params=PARAMS,
        name="rest",
    )(weights[:1], others, states)
    second = send(out)
    result = []
    for some, received in ((early, first), (late, second)):
        fresh = not result
        result = [
            pl.pallas_call(
                lambda *refs, some=some, fresh=fresh: finish_kernel(
                    *refs, groups=some, channels=channels, steps=steps, fresh=fresh
                ),
                out_shape=jax.ShapeDtypeStruct((channels, steps), f32),
                in_specs=[hbm_spec] * len(result) + [VM] * groups,
                out_specs=hbm_spec,
                input_output_aliases={} if fresh else {0: 0},
                scratch_shapes=[
                    pltpu.VMEM((channels, size(some)), f32),
                    pltpu.SemaphoreType.DMA((portions,)),
                ],
                compiler_params=PARAMS,
                name="finish",
            )(*result, own, *received)
        ]
    return result[0]


def solution(mesh):
    in_specs = (
        P(None, "chan", "tm"),
        P(None, "chan", "tm"),
        P(None, "chan", "tm"),
        P("chan", None, None),
    )
    out_specs = P("chan", "tm")
    return jax.shard_map(
        on_device, mesh=mesh, in_specs=in_specs, out_specs=out_specs, check_vma=False
    )
```

```python
import jax
import jax.numpy as jnp
from jax import lax
from jax.experimental import pallas as pl
from jax.experimental.pallas import tpu as pltpu
from jax.sharding import PartitionSpec as P

epsilon = 1e-06
LANES = 128
SUBS = 8


def cmul(a, b):
    return (a[0] * b[0] - a[1] * b[1], a[0] * b[1] + a[1] * b[0])


def conj_mul(a, b):
    return (a[0] * b[0] + a[1] * b[1], a[0] * b[1] - a[1] * b[0])


def cadd(a, b):
    return (a[0] + b[0], a[1] + b[1])


def row(x, s):
    return jnp.broadcast_to(x[s : s + 1, :], (SUBS, LANES))


def digits(devices):
    found = []
    while devices > 1:
        base = 4 if devices % 4 == 0 else 2 if devices % 2 == 0 else devices
        found.append(base)
        devices //= base
    return found


def slot_of(j, here, devices):
    slot, stride = 0, 1
    for base in digits(devices):
        if base & (base - 1):
            away = (here // stride % base - j // stride % base + base) % base
        else:
            shift = stride.bit_length() - 1
            away = ((here >> shift) - (j >> shift)) & (base - 1)
        slot = slot + stride * away
        stride *= base
    return slot


def gather_stages(msg, devices):
    parts, stride = [msg], 1
    for base in digits(devices):
        buf = jnp.concatenate(parts, axis=0) if len(parts) > 1 else parts[0]
        parts = [buf]
        for k in range(1, base):
            pairs = []
            for j in range(devices):
                d = j // stride % base
                pairs.append((j, j + ((d + k) % base - d) * stride))
            parts.append(lax.ppermute(buf, "tm", pairs))
        stride *= base
    return parts


def scan_kernel(
    side, trans, drive, back, readout, w, chunk, msg, weights, raw, table, sems, *, channels, steps
):
    portions = LANES // channels
    span = steps // portions
    length = span // SUBS
    pitch = length + 1
    piece = min(length, LANES)
    sources = (trans.at[0], trans.at[2], drive.at[0], drive.at[1], back.at[0], back.at[1])
    copies = [pltpu.make_async_copy(s, raw.at[k], sems.at[k]) for k, s in enumerate(sources)]
    copies.append(pltpu.make_async_copy(readout, table, sems.at[len(sources)]))
    for copy in copies:
        copy.start()
    def arrive(k):
        copies[k].wait()
        for g in range(span // LANES):
            x = jnp.concatenate(
                [raw[k, :, pl.ds(q * span + g * LANES, LANES)] for q in range(portions)], axis=0
            )
            xt = x.T
            for first in range(0, LANES, piece):
                r = g * LANES + first
                w[k, pl.ds((r // length) * pitch + r % length, piece), :] = xt[first : first + piece]


    for k in range(4):
        arrive(k)
    zero = jnp.zeros((SUBS, LANES), jnp.float32)
    one = jnp.ones((SUBS, LANES), jnp.float32)

    def at(k, t):
        return w[k, pl.ds(t, SUBS, stride=pitch), :]

    def advance(c, z, source, times):
        p, f, a, b, s = c
        p = times(z, p)
        f = cadd(times(z, f), source)
        a = a + (f[0] * f[0] + f[1] * f[1])
        b = cadd(b, conj_mul(p, f))
        s = s + (p[0] * p[0] + p[1] * p[1])
        return p, f, a, b, s

    def forward(i, c):
        return advance(c, (at(0, i), at(1, i)), (at(2, i), at(3, i)), cmul)

    def backward(i, c):
        j = length - 1 - i
        return advance(c, (at(0, j), at(1, j)), (at(4, j), at(5, j)), conj_mul)

    nil = (zero, zero)
    unit = (one, zero)
    begin = (unit, nil, zero, nil, zero)
    p, f, af, bf, cf = lax.fori_loop(0, length, forward, begin, unroll=8)
    arrive(4)
    arrive(5)
    q, g, ab, bb, cb = lax.fori_loop(0, length, backward, begin, unroll=8)
    copies[-1].wait()
    low = lax.broadcasted_iota(jnp.int32, (channels, LANES), 1) < channels
    for t in range(weights.shape[0]):
        other = (side[0] + t) % weights.shape[0]
        for k in range(2):
            shifted = pltpu.roll(table[:, k, :], (LANES - other * channels) % LANES, 1)
            weights[t, k] = jnp.where(low, shifted, 0.0)

    sub = lax.broadcasted_iota(jnp.int32, (SUBS, LANES), 0)
    portion = lax.broadcasted_iota(jnp.int32, (SUBS, LANES), 1) // channels

    def pick(mask, a, b):
        return tuple(jnp.where(mask, x, y) for x, y in zip(a, b))

    def spread(v):
        total = v
        for m in range(1, portions):
            total = total + pltpu.roll(v, m * channels, 1)
        return total

    def combine(m, v, order, edge, shift):
        start, product = nil, unit
        base_v, base_m = nil, unit
        for s in order:
            base_v = pick(sub == s, start, base_v)
            base_m = pick(sub == s, product, base_m)
            ms, vs = (row(m[0], s), row(m[1], s)), (row(v[0], s), row(v[1], s))
            start = cadd(cmul(ms, start), vs)
            product = cmul(ms, product)
        ex_v, ex_m = nil, unit
        for _ in range(portions - 1):
            nv, nm = cadd(cmul(product, ex_v), start), cmul(product, ex_m)
            nv = tuple(pltpu.roll(a, shift, 1) for a in nv)
            nm = tuple(pltpu.roll(a, shift, 1) for a in nm)
            ex_v, ex_m = pick(portion == edge, nil, nv), pick(portion == edge, unit, nm)
        base_v = cadd(base_v, cmul(base_m, ex_v))
        base_m = cmul(base_m, ex_m)
        total_v, total_m = cadd(cmul(product, ex_v), start), cmul(product, ex_m)
        last = portion == portions - 1 - edge
        total_v = tuple(spread(jnp.where(last, a, zero)) for a in total_v)
        total_m = tuple(spread(jnp.where(last, a, zero)) for a in total_m)
        return base_v, base_m, total_v, total_m

    def stats(a, b, c, v, m):
        cross = conj_mul(v, b)
        whole = a + 2.0 * cross[0] + (v[0] * v[0] + v[1] * v[1]) * c
        mixed = conj_mul(m, (b[0] + c * v[0], b[1] + c * v[1]))
        square = (m[0] * m[0] + m[1] * m[1]) * c
        return tuple(
            spread(jnp.broadcast_to(jnp.sum(x, axis=0, keepdims=True), (SUBS, LANES)))
            for x in (whole, mixed[0], mixed[1], square)
        )

    f0, p0, fe, pe = combine(p, f, range(SUBS), 0, channels)
    g0, q0, ge, _ = combine(
        q, g, range(SUBS - 1, -1, -1), portions - 1, (LANES - channels) % LANES
    )
    for k, x in enumerate(f0 + p0 + g0 + q0):
        chunk[k] = x
    rows = pe + fe + ge + stats(af, bf, cf, f0, p0) + stats(ab, bb, cb, g0, q0)
    for half in range(2):
        block = zero
        for s, x in enumerate(rows[half * SUBS : (half + 1) * SUBS]):
            block = jnp.where(sub == s, x, block)
        msg[half * SUBS : (half + 1) * SUBS, :] = block


def readout_rows(weights, s_ref, out, target, groups, *, channels, steps):
    portions = LANES // channels
    span = steps // portions
    length = span // SUBS
    pitch = length + 1
    piece = min(length, LANES)
    left = jnp.concatenate(
        [
            jnp.concatenate(
                [pltpu.roll(weights[k], q * channels, 1) if q else weights[k] for q in range(portions)],
                axis=0,
            )
            for k in range(2)
        ],
        axis=1,
    )

    def split(x):
        high = x.astype(jnp.bfloat16)
        return high, (x - high.astype(jnp.float32)).astype(jnp.bfloat16)

    def dot(a, b):
        return lax.dot_general(a, b, (((1,), (1,)), ((), ())), preferred_element_type=jnp.float32)

    left_high, left_low = split(left)
    width = len(groups) * LANES
    for g in groups:
        parts = []
        for k in range(2):
            rows = []
            for first in range(0, LANES, piece):
                r = g * LANES + first
                rows.append(s_ref[k, pl.ds((r // length) * pitch + r % length, piece), :])
            parts.append(jnp.concatenate(rows, axis=0) if len(rows) > 1 else rows[0])
        high, low = split(jnp.concatenate(parts, axis=1))
        res = dot(left_high, high) + (dot(left_high, low) + dot(left_low, high))
        for q in range(portions):
            column = q * width + (g - groups[0]) * LANES
            out[target, :, pl.ds(column, LANES)] = res[q * channels : (q + 1) * channels]


def state_kernel(place, chunk, w, *rest, groups, channels, steps, devices):
    parts, weights, (out, s_ref, gath) = rest[:-4], rest[-4], rest[-3:]
    for k, part in enumerate(parts):
        size = part.shape[0]
        gath[k * size : (k + 1) * size, :] = part[...]
    portions = LANES // channels
    length = steps // portions // SUBS
    pitch = length + 1
    here = place[0]

    def take(j, r):
        return gath[pl.ds(slot_of(j, here, devices) * 16 + r, 1), :]

    def full(x):
        return jnp.broadcast_to(x, (SUBS, LANES))

    def square(j, base, v):
        cross = conj_mul(v, (take(j, base + 1), take(j, base + 2)))
        return (
            take(j, base) + 2.0 * cross[0] + (v[0] * v[0] + v[1] * v[1]) * take(j, base + 3)
        )

    def walk(j, c):
        f, mine_f, sum_f, g, mine_g, sum_g = c
        sum_f = sum_f + square(j, 6, f)
        mine_f = tuple(jnp.where(j == here, a, b) for a, b in zip(f, mine_f))
        f = cadd(cmul((take(j, 0), take(j, 1)), f), (take(j, 2), take(j, 3)))
        i = devices - 1 - j
        sum_g = sum_g + square(i, 10, g)
        mine_g = tuple(jnp.where(i == here, a, b) for a, b in zip(g, mine_g))
        g = cadd(conj_mul((take(i, 0), take(i, 1)), g), (take(i, 4), take(i, 5)))
        return f, mine_f, sum_f, g, mine_g, sum_g

    last = devices - 1
    f, g = (take(0, 2), take(0, 3)), (take(last, 4), take(last, 5))
    _, f, sum_f, _, g, sum_g = lax.fori_loop(
        1, devices, walk, (f, f, take(0, 6), g, g, take(last, 10)), unroll=5
    )
    f = tuple(jnp.where(here == 0, 0.0, a) for a in f)
    g = tuple(jnp.where(here == last, 0.0, a) for a in g)
    count = 2.0 * steps * devices
    scale_f = full(1.0 / jnp.sqrt(sum_f / count + epsilon))
    scale_g = full(1.0 / jnp.sqrt(sum_g / count + epsilon))
    f, g = tuple(map(full, f)), tuple(map(full, g))
    f = cadd((chunk[0], chunk[1]), cmul((chunk[2], chunk[3]), f))
    g = cadd((chunk[4], chunk[5]), cmul((chunk[6], chunk[7]), g))
    half = length // 2

    def step(i, c, later):
        f, g = c
        at = lambda k, t: w[k, pl.ds(t, SUBS, stride=pitch), :]
        j = length - 1 - i
        f = cadd(cmul((at(0, i), at(1, i)), f), (at(2, i), at(3, i)))
        g = cadd(conj_mul((at(0, j), at(1, j)), g), (at(4, j), at(5, j)))
        for k in range(2):
            a = f[k] * scale_f
            b = g[k] * scale_g
            if later:
                a = a + s_ref[k, pl.ds(i, SUBS, stride=pitch), :]
                b = b + s_ref[k, pl.ds(j, SUBS, stride=pitch), :]
            s_ref[k, pl.ds(i, SUBS, stride=pitch), :] = a
            s_ref[k, pl.ds(j, SUBS, stride=pitch), :] = b
        return f, g

    c = lax.fori_loop(0, half, lambda i, c: step(i, c, False), (f, g), unroll=8)
    lax.fori_loop(half, length, lambda i, c: step(i, c, True), c, unroll=8)
    for t in range(weights.shape[0]):
        readout_rows(weights.at[t], s_ref, out, t, groups, channels=channels, steps=steps)


def rest_kernel(weights, others, s_ref, out, own, *, groups, channels, steps):
    for t in range(others.shape[0]):
        readout_rows(others.at[t], s_ref, out, t, groups, channels=channels, steps=steps)
    every = range(groups[-1] + 1)
    readout_rows(weights.at[0], s_ref, own, 0, every, channels=channels, steps=steps)


def finish_kernel(*refs, groups, channels, steps, fresh):
    own, *received, out, total, sems = refs if fresh else refs[1:]
    portions = LANES // channels
    span = steps // portions
    width = len(groups) * LANES
    copies = []
    for q in range(portions):
        there = pl.ds(q * span + groups[0] * LANES, width)
        here = pl.ds(q * width, width)
        value = own[0, :, there]
        for part in received:
            value = value + part[:, here]
        total[:, here] = value
        copies.append(pltpu.make_async_copy(total.at[:, here], out.at[:, there], sems.at[q]))
        copies[-1].start()
    for copy in copies:
        copy.wait()


VM = pl.BlockSpec(memory_space=pltpu.VMEM)
PARAMS = pltpu.CompilerParams(vmem_limit_bytes=40 * 1024 * 1024)


def on_device(trans, drive, back_drive, readout):
    channels = trans.shape[1]
    steps = trans.shape[2]
    devices = lax.axis_size("tm")
    groups = lax.axis_size("chan")
    portions = LANES // channels
    length = steps // portions // SUBS
    rows = SUBS * (length + 1)
    rows = (rows + 7) // 8 * 8
    here = lax.axis_index("chan")
    f32 = jnp.float32

    hbm_spec = pl.BlockSpec(memory_space=pltpu.HBM)
    smem_spec = pl.BlockSpec(memory_space=pltpu.SMEM)
    trans, drive, back_drive, readout = (
        pltpu.with_memory_space_constraint(x, pltpu.HBM)
        for x in (trans, drive, back_drive, readout)
    )
    w, chunk, msg, weights = pl.pallas_call(
        lambda *refs: scan_kernel(*refs, channels=channels, steps=steps),
        out_shape=(
            jax.ShapeDtypeStruct((6, rows, LANES), f32),
            jax.ShapeDtypeStruct((8, SUBS, LANES), f32),
            jax.ShapeDtypeStruct((16, LANES), f32),
            jax.ShapeDtypeStruct((groups, 2, channels, LANES), f32),
        ),
        in_specs=[smem_spec] + [hbm_spec] * 4,
        out_specs=(VM, VM, VM, VM),
        scratch_shapes=[
            pltpu.VMEM((6, channels, steps), f32),
            pltpu.VMEM(readout.shape, f32),
            pltpu.SemaphoreType.DMA((7,)),
        ],
        compiler_params=PARAMS,
        name="local_scan",
    )(here.reshape(1).astype(jnp.int32), trans, drive, back_drive, readout)
    parts = gather_stages(msg, devices)
    others = []
    for k in range(1, groups):
        pairs = [(j, (j + k) % groups) for j in range(groups)]
        others.append(lax.ppermute(weights[k], "chan", pairs))
    place = lax.axis_index("tm").reshape(1).astype(jnp.int32)
    pieces = steps // portions // LANES
    tail = max(1, pieces // 4)
    early, late = range(pieces - tail), range(pieces - tail, pieces)
    size = lambda some: len(some) * LANES * portions
    others = jnp.stack(others)
    out, states = pl.pallas_call(
        lambda *refs: state_kernel(
            *refs, groups=early, channels=channels, steps=steps, devices=devices
        ),
        out_shape=(
            jax.ShapeDtypeStruct((groups - 1, channels, size(early)), f32),
            jax.ShapeDtypeStruct((2, rows, LANES), f32),
        ),
        in_specs=[smem_spec] + [VM] * (3 + len(parts)),
        out_specs=(VM, VM),
        scratch_shapes=[pltpu.VMEM((16 * devices, LANES), f32)],
        compiler_params=PARAMS,
        name="states",
    )(place, chunk, w, *parts, others)

    def send(values):
        received = []
        for k in range(1, groups):
            pairs = [(j, (j - k) % groups) for j in range(groups)]
            received.append(lax.ppermute(values[k - 1], "chan", pairs))
        return received

    first = send(out)
    out, own = pl.pallas_call(
        lambda *refs: rest_kernel(*refs, groups=late, channels=channels, steps=steps),
        out_shape=(
            jax.ShapeDtypeStruct((groups - 1, channels, size(late)), f32),
            jax.ShapeDtypeStruct((1, channels, steps), f32),
        ),
        in_specs=[VM, VM, VM],
        out_specs=(VM, VM),
        compiler_params=PARAMS,
        name="rest",
    )(weights[:1], others, states)
    second = send(out)
    result = []
    for some, received in ((early, first), (late, second)):
        fresh = not result
        result = [
            pl.pallas_call(
                lambda *refs, some=some, fresh=fresh: finish_kernel(
                    *refs, groups=some, channels=channels, steps=steps, fresh=fresh
                ),
                out_shape=jax.ShapeDtypeStruct((channels, steps), f32),
                in_specs=[hbm_spec] * len(result) + [VM] * groups,
                out_specs=hbm_spec,
                input_output_aliases={} if fresh else {0: 0},
                scratch_shapes=[
                    pltpu.VMEM((channels, size(some)), f32),
                    pltpu.SemaphoreType.DMA((portions,)),
                ],
                compiler_params=PARAMS,
                name="finish",
            )(*result, own, *received)
        ]
    return result[0]


def solution(mesh):
    in_specs = (
        P(None, "chan", "tm"),
        P(None, "chan", "tm"),
        P(None, "chan", "tm"),
        P("chan", None, None),
    )
    out_specs = P("chan", "tm")
    return jax.shard_map(
        on_device, mesh=mesh, in_specs=in_specs, out_specs=out_specs, check_vma=False
    )
```

```python
import jax
import jax.numpy as jnp
from jax import lax
from jax.experimental import pallas as pl
from jax.experimental.pallas import tpu as pltpu
from jax.sharding import PartitionSpec as P

epsilon = 1e-06
LANES = 128
SUBS = 8


def cmul(a, b):
    return (a[0] * b[0] - a[1] * b[1], a[0] * b[1] + a[1] * b[0])


def conj_mul(a, b):
    return (a[0] * b[0] + a[1] * b[1], a[0] * b[1] - a[1] * b[0])


def cadd(a, b):
    return (a[0] + b[0], a[1] + b[1])


def row(x, s):
    return jnp.broadcast_to(x[s : s + 1, :], (SUBS, LANES))


def digits(devices):
    found = []
    while devices > 1:
        base = 4 if devices % 4 == 0 else 2 if devices % 2 == 0 else devices
        found.append(base)
        devices //= base
    return found


def slot_of(j, here, devices):
    slot, stride = 0, 1
    for base in digits(devices):
        if base & (base - 1):
            away = (here // stride % base - j // stride % base + base) % base
        else:
            shift = stride.bit_length() - 1
            away = ((here >> shift) - (j >> shift)) & (base - 1)
        slot = slot + stride * away
        stride *= base
    return slot


def gather_stages(msg, devices):
    parts, stride = [msg], 1
    for base in digits(devices):
        buf = jnp.concatenate(parts, axis=0) if len(parts) > 1 else parts[0]
        parts = [buf]
        for k in range(1, base):
            pairs = []
            for j in range(devices):
                d = j // stride % base
                pairs.append((j, j + ((d + k) % base - d) * stride))
            parts.append(lax.ppermute(buf, "tm", pairs))
        stride *= base
    return parts


def scan_kernel(
    side, trans, drive, back, readout, w, chunk, msg, weights, raw, table, sems, *, channels, steps
):
    portions = LANES // channels
    span = steps // portions
    length = span // SUBS
    pitch = length + 1
    piece = min(length, LANES)
    sources = (trans.at[0], trans.at[2], drive.at[0], drive.at[1], back.at[0], back.at[1])
    copies = [pltpu.make_async_copy(s, raw.at[k], sems.at[k]) for k, s in enumerate(sources)]
    copies.append(pltpu.make_async_copy(readout, table, sems.at[len(sources)]))
    for copy in copies:
        copy.start()
    for k, copy in enumerate(copies[:-1]):
        copy.wait()
        for g in range(span // LANES):
            x = jnp.concatenate(
                [raw[k, :, pl.ds(q * span + g * LANES, LANES)] for q in range(portions)], axis=0
            )
            xt = x.T
            for first in range(0, LANES, piece):
                r = g * LANES + first
                w[k, pl.ds((r // length) * pitch + r % length, piece), :] = xt[first : first + piece]

    copies[-1].wait()
    low = lax.broadcasted_iota(jnp.int32, (channels, LANES), 1) < channels
    for t in range(weights.shape[0]):
        other = (side[0] + t) % weights.shape[0]
        for k in range(2):
            shifted = pltpu.roll(table[:, k, :], (LANES - other * channels) % LANES, 1)
            weights[t, k] = jnp.where(low, shifted, 0.0)

    zero = jnp.zeros((SUBS, LANES), jnp.float32)
    one = jnp.ones((SUBS, LANES), jnp.float32)

    def step(i, c):
        p, f, q, g, af, bf, cf, ab, bb, cb = c
        at = lambda k, t: w[k, pl.ds(t, SUBS, stride=pitch), :]
        z = (at(0, i), at(1, i))
        p = cmul(z, p)
        f = cadd(cmul(z, f), (at(2, i), at(3, i)))
        af = af + (f[0] * f[0] + f[1] * f[1])
        bf = cadd(bf, conj_mul(p, f))
        cf = cf + (p[0] * p[0] + p[1] * p[1])
        j = length - 1 - i
        y = (at(0, j), at(1, j))
        q = conj_mul(y, q)
        g = cadd(conj_mul(y, g), (at(4, j), at(5, j)))
        ab = ab + (g[0] * g[0] + g[1] * g[1])
        bb = cadd(bb, conj_mul(q, g))
        cb = cb + (q[0] * q[0] + q[1] * q[1])
        return p, f, q, g, af, bf, cf, ab, bb, cb

    nil = (zero, zero)
    unit = (one, zero)
    p, f, q, g, af, bf, cf, ab, bb, cb = lax.fori_loop(
        0, length, step, (unit, nil, unit, nil, zero, nil, zero, zero, nil, zero), unroll=8
    )

    sub = lax.broadcasted_iota(jnp.int32, (SUBS, LANES), 0)
    portion = lax.broadcasted_iota(jnp.int32, (SUBS, LANES), 1) // channels

    def pick(mask, a, b):
        return tuple(jnp.where(mask, x, y) for x, y in zip(a, b))

    def spread(v):
        total = v
        for m in range(1, portions):
            total = total + pltpu.roll(v, m * channels, 1)
        return total

    def combine(m, v, order, edge, shift):
        start, product = nil, unit
        base_v, base_m = nil, unit
        for s in order:
            base_v = pick(sub == s, start, base_v)
            base_m = pick(sub == s, product, base_m)
            ms, vs = (row(m[0], s), row(m[1], s)), (row(v[0], s), row(v[1], s))
            start = cadd(cmul(ms, start), vs)
            product = cmul(ms, product)
        ex_v, ex_m = nil, unit
        for _ in range(portions - 1):
            nv, nm = cadd(cmul(product, ex_v), start), cmul(product, ex_m)
            nv = tuple(pltpu.roll(a, shift, 1) for a in nv)
            nm = tuple(pltpu.roll(a, shift, 1) for a in nm)
            ex_v, ex_m = pick(portion == edge, nil, nv), pick(portion == edge, unit, nm)
        base_v = cadd(base_v, cmul(base_m, ex_v))
        base_m = cmul(base_m, ex_m)
        total_v, total_m = cadd(cmul(product, ex_v), start), cmul(product, ex_m)
        last = portion == portions - 1 - edge
        total_v = tuple(spread(jnp.where(last, a, zero)) for a in total_v)
        total_m = tuple(spread(jnp.where(last, a, zero)) for a in total_m)
        return base_v, base_m, total_v, total_m

    def stats(a, b, c, v, m):
        cross = conj_mul(v, b)
        whole = a + 2.0 * cross[0] + (v[0] * v[0] + v[1] * v[1]) * c
        mixed = conj_mul(m, (b[0] + c * v[0], b[1] + c * v[1]))
        square = (m[0] * m[0] + m[1] * m[1]) * c
        return tuple(
            spread(jnp.broadcast_to(jnp.sum(x, axis=0, keepdims=True), (SUBS, LANES)))
            for x in (whole, mixed[0], mixed[1], square)
        )

    f0, p0, fe, pe = combine(p, f, range(SUBS), 0, channels)
    g0, q0, ge, _ = combine(
        q, g, range(SUBS - 1, -1, -1), portions - 1, (LANES - channels) % LANES
    )
    for k, x in enumerate(f0 + p0 + g0 + q0):
        chunk[k] = x
    rows = pe + fe + ge + stats(af, bf, cf, f0, p0) + stats(ab, bb, cb, g0, q0)
    for half in range(2):
        block = zero
        for s, x in enumerate(rows[half * SUBS : (half + 1) * SUBS]):
            block = jnp.where(sub == s, x, block)
        msg[half * SUBS : (half + 1) * SUBS, :] = block


def readout_rows(weights, s_ref, out, target, groups, *, channels, steps):
    portions = LANES // channels
    span = steps // portions
    length = span // SUBS
    pitch = length + 1
    piece = min(length, LANES)
    left = jnp.concatenate(
        [
            jnp.concatenate(
                [pltpu.roll(weights[k], q * channels, 1) if q else weights[k] for q in range(portions)],
                axis=0,
            )
            for k in range(2)
        ],
        axis=1,
    )

    def split(x):
        high = x.astype(jnp.bfloat16)
        return high, (x - high.astype(jnp.float32)).astype(jnp.bfloat16)

    def dot(a, b):
        return lax.dot_general(a, b, (((1,), (1,)), ((), ())), preferred_element_type=jnp.float32)

    left_high, left_low = split(left)
    width = len(groups) * LANES
    for g in groups:
        parts = []
        for k in range(2):
            rows = []
            for first in range(0, LANES, piece):
                r = g * LANES + first
                rows.append(s_ref[k, pl.ds((r // length) * pitch + r % length, piece), :])
            parts.append(jnp.concatenate(rows, axis=0) if len(rows) > 1 else rows[0])
        high, low = split(jnp.concatenate(parts, axis=1))
        res = dot(left_high, high) + (dot(left_high, low) + dot(left_low, high))
        for q in range(portions):
            column = q * width + (g - groups[0]) * LANES
            out[target, :, pl.ds(column, LANES)] = res[q * channels : (q + 1) * channels]


def state_kernel(place, chunk, w, *rest, groups, channels, steps, devices):
    parts, weights, (out, s_ref, gath) = rest[:-4], rest[-4], rest[-3:]
    for k, part in enumerate(parts):
        size = part.shape[0]
        gath[k * size : (k + 1) * size, :] = part[...]
    portions = LANES // channels
    length = steps // portions // SUBS
    pitch = length + 1
    here = place[0]

    def take(j, r):
        return gath[pl.ds(slot_of(j, here, devices) * 16 + r, 1), :]

    def full(x):
        return jnp.broadcast_to(x, (SUBS, LANES))

    def square(j, base, v):
        cross = conj_mul(v, (take(j, base + 1), take(j, base + 2)))
        return (
            take(j, base) + 2.0 * cross[0] + (v[0] * v[0] + v[1] * v[1]) * take(j, base + 3)
        )

    def walk(j, c):
        f, mine_f, sum_f, g, mine_g, sum_g = c
        sum_f = sum_f + square(j, 6, f)
        mine_f = tuple(jnp.where(j == here, a, b) for a, b in zip(f, mine_f))
        f = cadd(cmul((take(j, 0), take(j, 1)), f), (take(j, 2), take(j, 3)))
        i = devices - 1 - j
        sum_g = sum_g + square(i, 10, g)
        mine_g = tuple(jnp.where(i == here, a, b) for a, b in zip(g, mine_g))
        g = cadd(conj_mul((take(i, 0), take(i, 1)), g), (take(i, 4), take(i, 5)))
        return f, mine_f, sum_f, g, mine_g, sum_g

    last = devices - 1
    f, g = (take(0, 2), take(0, 3)), (take(last, 4), take(last, 5))
    _, f, sum_f, _, g, sum_g = lax.fori_loop(
        1, devices, walk, (f, f, take(0, 6), g, g, take(last, 10)), unroll=5
    )
    f = tuple(jnp.where(here == 0, 0.0, a) for a in f)
    g = tuple(jnp.where(here == last, 0.0, a) for a in g)
    count = 2.0 * steps * devices
    scale_f = full(1.0 / jnp.sqrt(sum_f / count + epsilon))
    scale_g = full(1.0 / jnp.sqrt(sum_g / count + epsilon))
    f, g = tuple(map(full, f)), tuple(map(full, g))
    f = cadd((chunk[0], chunk[1]), cmul((chunk[2], chunk[3]), f))
    g = cadd((chunk[4], chunk[5]), cmul((chunk[6], chunk[7]), g))
    half = length // 2

    def step(i, c, later):
        f, g = c
        at = lambda k, t: w[k, pl.ds(t, SUBS, stride=pitch), :]
        j = length - 1 - i
        f = cadd(cmul((at(0, i), at(1, i)), f), (at(2, i), at(3, i)))
        g = cadd(conj_mul((at(0, j), at(1, j)), g), (at(4, j), at(5, j)))
        for k in range(2):
            a = f[k] * scale_f
            b = g[k] * scale_g
            if later:
                a = a + s_ref[k, pl.ds(i, SUBS, stride=pitch), :]
                b = b + s_ref[k, pl.ds(j, SUBS, stride=pitch), :]
            s_ref[k, pl.ds(i, SUBS, stride=pitch), :] = a
            s_ref[k, pl.ds(j, SUBS, stride=pitch), :] = b
        return f, g

    c = lax.fori_loop(0, half, lambda i, c: step(i, c, False), (f, g), unroll=8)
    lax.fori_loop(half, length, lambda i, c: step(i, c, True), c, unroll=8)
    for t in range(weights.shape[0]):
        readout_rows(weights.at[t], s_ref, out, t, groups, channels=channels, steps=steps)


def rest_kernel(weights, others, s_ref, out, own, *, groups, channels, steps):
    for t in range(others.shape[0]):
        readout_rows(others.at[t], s_ref, out, t, groups, channels=channels, steps=steps)
    every = range(groups[-1] + 1)
    readout_rows(weights.at[0], s_ref, own, 0, every, channels=channels, steps=steps)


def finish_kernel(*refs, groups, channels, steps, fresh):
    own, *received, out, total, sems = refs if fresh else refs[1:]
    portions = LANES // channels
    span = steps // portions
    width = len(groups) * LANES
    copies = []
    for q in range(portions):
        there = pl.ds(q * span + groups[0] * LANES, width)
        here = pl.ds(q * width, width)
        value = own[0, :, there]
        for part in received:
            value = value + part[:, here]
        total[:, here] = value
        copies.append(pltpu.make_async_copy(total.at[:, here], out.at[:, there], sems.at[q]))
        copies[-1].start()
    for copy in copies:
        copy.wait()


VM = pl.BlockSpec(memory_space=pltpu.VMEM)
PARAMS = pltpu.CompilerParams(vmem_limit_bytes=40 * 1024 * 1024)


def on_device(trans, drive, back_drive, readout):
    channels = trans.shape[1]
    steps = trans.shape[2]
    devices = lax.axis_size("tm")
    groups = lax.axis_size("chan")
    portions = LANES // channels
    length = steps // portions // SUBS
    rows = SUBS * (length + 1)
    rows = (rows + 7) // 8 * 8
    here = lax.axis_index("chan")
    f32 = jnp.float32

    hbm_spec = pl.BlockSpec(memory_space=pltpu.HBM)
    smem_spec = pl.BlockSpec(memory_space=pltpu.SMEM)
    trans, drive, back_drive, readout = (
        pltpu.with_memory_space_constraint(x, pltpu.HBM)
        for x in (trans, drive, back_drive, readout)
    )
    w, chunk, msg, weights = pl.pallas_call(
        lambda *refs: scan_kernel(*refs, channels=channels, steps=steps),
        out_shape=(
            jax.ShapeDtypeStruct((6, rows, LANES), f32),
            jax.ShapeDtypeStruct((8, SUBS, LANES), f32),
            jax.ShapeDtypeStruct((16, LANES), f32),
            jax.ShapeDtypeStruct((groups, 2, channels, LANES), f32),
        ),
        in_specs=[smem_spec] + [hbm_spec] * 4,
        out_specs=(VM, VM, VM, VM),
        scratch_shapes=[
            pltpu.VMEM((6, channels, steps), f32),
            pltpu.VMEM(readout.shape, f32),
            pltpu.SemaphoreType.DMA((7,)),
        ],
        compiler_params=PARAMS,
        name="local_scan",
    )(here.reshape(1).astype(jnp.int32), trans, drive, back_drive, readout)
    parts = gather_stages(msg, devices)
    others = []
    for k in range(1, groups):
        pairs = [(j, (j + k) % groups) for j in range(groups)]
        tied, _ = lax.optimization_barrier((weights[k], parts[0]))
        others.append(lax.ppermute(tied, "chan", pairs))
    place = lax.axis_index("tm").reshape(1).astype(jnp.int32)
    pieces = steps // portions // LANES
    tail = max(1, pieces // 4)
    early, late = range(pieces - tail), range(pieces - tail, pieces)
    size = lambda some: len(some) * LANES * portions
    others = jnp.stack(others)
    out, states = pl.pallas_call(
        lambda *refs: state_kernel(
            *refs, groups=early, channels=channels, steps=steps, devices=devices
        ),
        out_shape=(
            jax.ShapeDtypeStruct((groups - 1, channels, size(early)), f32),
            jax.ShapeDtypeStruct((2, rows, LANES), f32),
        ),
        in_specs=[smem_spec] + [VM] * (3 + len(parts)),
        out_specs=(VM, VM),
        scratch_shapes=[pltpu.VMEM((16 * devices, LANES), f32)],
        compiler_params=PARAMS,
        name="states",
    )(place, chunk, w, *parts, others)

    def send(values):
        received = []
        for k in range(1, groups):
            pairs = [(j, (j - k) % groups) for j in range(groups)]
            received.append(lax.ppermute(values[k - 1], "chan", pairs))
        return received

    first = send(out)
    out, own = pl.pallas_call(
        lambda *refs: rest_kernel(*refs, groups=late, channels=channels, steps=steps),
        out_shape=(
            jax.ShapeDtypeStruct((groups - 1, channels, size(late)), f32),
            jax.ShapeDtypeStruct((1, channels, steps), f32),
        ),
        in_specs=[VM, VM, VM],
        out_specs=(VM, VM),
        compiler_params=PARAMS,
        name="rest",
    )(weights[:1], others, states)
    second = send(out)
    result = []
    for some, received in ((early, first), (late, second)):
        fresh = not result
        result = [
            pl.pallas_call(
                lambda *refs, some=some, fresh=fresh: finish_kernel(
                    *refs, groups=some, channels=channels, steps=steps, fresh=fresh
                ),
                out_shape=jax.ShapeDtypeStruct((channels, steps), f32),
                in_specs=[hbm_spec] * len(result) + [VM] * groups,
                out_specs=hbm_spec,
                input_output_aliases={} if fresh else {0: 0},
                scratch_shapes=[
                    pltpu.VMEM((channels, size(some)), f32),
                    pltpu.SemaphoreType.DMA((portions,)),
                ],
                compiler_params=PARAMS,
                name="finish",
            )(*result, own, *received)
        ]
    return result[0]


def solution(mesh):
    in_specs = (
        P(None, "chan", "tm"),
        P(None, "chan", "tm"),
        P(None, "chan", "tm"),
        P("chan", None, None),
    )
    out_specs = P("chan", "tm")
    return jax.shard_map(
        on_device, mesh=mesh, in_specs=in_specs, out_specs=out_specs, check_vma=False
    )
```
